32 devices in a mesh: row: 8 (over z, core), col: 4 (over y, x).
Axes of the slice: x: 2, y: 2, z: 4, core: 2. Of those that a mesh axis runs over, the one named last changes fastest.
Arguments:
- gate_input: bfloat16 [2, 512, 53248], P(None, 'col', 'row'), may hold values from -6 to 6
- up_input: bfloat16 [2, 512, 53248], P(None, 'col', 'row'), may hold values from -6 to 6
- down_weight: bfloat16 [53248, 16384], P('row', 'col'), may hold values from -0.02734375 to 0.02734375
Outputs:
- mixed: bfloat16 [2, 512, 16384], P(None, 'row', 'col')
The draws below stay inside these ranges and needn't reach their ends.
All inputs are finite; a program needn't handle non-finite values.
Results may differ from the reference program's by a relative error of at most 0.0049.
Values may be sent and summed in bfloat16 or wider, within the bound.
No kernel may reach another device: no remote copies, remote signals or barrier semaphores. Data moves between devices by JAX's collectives and lax.ppermute only.
A program may use at most 128 MiB of HBM per device.

```python
import jax
import jax.numpy as jnp

D = 16384
FF = 53248
SEQS = 2
MINISEQ = 512


def block_scale(key, dims, cuts, least, top_value):
    loudness = 1.0
    for axis_at, blocks in cuts:
        steps = jax.random.uniform(jax.random.fold_in(jax.random.fold_in(key, 6), axis_at), (blocks,), jnp.float32, least / len(cuts), top_value / len(cuts))
        loudness = loudness * jnp.repeat(jnp.exp(steps), dims[axis_at] // blocks).reshape((-1,) + (1,) * (len(dims) - 1 - axis_at))
    return loudness


def centred(own_key, shape, width, most, split=(), dtype=jnp.bfloat16):
    values = width * jax.random.normal(own_key, shape, jnp.float32)
    if split:
        values = values * block_scale(own_key, shape, split, -0.22, 0.18)
    return jnp.clip(values, -most, most).astype(dtype)


def setup_inputs(seed: int = 0) -> dict:
    key_of = jax.random.split(jax.random.key(seed), 4)
    gate_input = centred(key_of[0], (SEQS, MINISEQ, FF), 1.0, 6.0, ((1, 4), (2, 8)))
    up_input = centred(key_of[1], (SEQS, MINISEQ, FF), 1.0, 6.0, ((1, 4), (2, 8)))
    down_weight = centred(key_of[2], (FF, D), FF ** -0.5, 0.02734375, ((0, 8), (1, 4)))
    return dict(gate_input=gate_input, up_input=up_input, down_weight=down_weight)


def reference(gate_input, up_input, down_weight):
    hidden = (jax.nn.silu(gate_input.astype(jnp.float32)) * up_input.astype(jnp.float32)).astype(jnp.bfloat16)
    flat = hidden.reshape(SEQS * MINISEQ, FF)
    mixed = jnp.dot(flat, down_weight, preferred_element_type=jnp.float32)
    return mixed.astype(jnp.bfloat16).reshape(SEQS, MINISEQ, D)
```

```python
import jax
import jax.numpy as jnp
from jax import lax
from jax.sharding import PartitionSpec as P


SIZES = (2, 3, 3)
LAST_CUTS = 2


def gated_hidden(gate_part, up_part):
    product = jax.nn.silu(gate_part.astype(jnp.float32)) * up_part.astype(jnp.float32)
    return product.astype(jnp.bfloat16)


def solution(mesh):
    n_row = mesh.shape["row"]
    n_col = mesh.shape["col"]
    share = n_row // n_col
    slow = 2 if n_col % 2 == 0 else 1
    fast = n_col // slow
    n = len(SIZES)

    def shift_slow(value, step):
        pairs = [(a * fast + b, (a + step) % slow * fast + b) for a in range(slow) for b in range(fast)]
        return lax.ppermute(value, "col", pairs)

    def shift_fast(value, step):
        pairs = [(a * fast + b, a * fast + (b + step) % fast) for a in range(slow) for b in range(fast)]
        return lax.ppermute(value, "col", pairs)

    def shift_part(value, step):
        pairs = [(z * share + k, z * share + (k + step) % share) for z in range(n_col) for k in range(share)]
        return lax.ppermute(value, "row", pairs)

    def shift_group(value, step):
        pairs = [(z * share + k, (z + step) % n_col * share + k) for z in range(n_col) for k in range(share)]
        return lax.ppermute(value, "row", pairs)

    def layer(gate_input, up_input, down_weight):
        seqs, tokens, units = gate_input.shape
        width = down_weight.shape[1]
        own = tokens // share
        rows = seqs * own
        half = units // 2
        row = lax.axis_index("row")
        col = lax.axis_index("col")
        group, part = row // share, row % share
        at_slow, at_fast = col // fast, col % fast
        edges = [rows * sum(SIZES[:i]) // sum(SIZES) for i in range(n + 1)]

        def place(source):
            return (at_slow - source // fast) % slow * fast + (at_fast - source % fast) % fast

        def hidden_of(lo, hi):
            hidden = gated_hidden(gate_input[:, :, lo:hi], up_input[:, :, lo:hi])
            hidden = hidden.reshape(seqs, share, own, hi - lo)
            return hidden.transpose(1, 0, 2, 3).reshape(share, rows, hi - lo)

        first = hidden_of(0, half)
        second = hidden_of(half, units)
        outs = {}
        for i in range(n):
            mine_first = first[:, edges[i]:edges[i + 1]]
            mine_second = second[:, edges[i]:edges[i + 1]]
            left, right = {(0, 0): mine_first}, {(0, 0): mine_second}
            for da in range(1, slow):
                left[da, 0] = shift_slow(mine_first, da)
            for db in range(1, fast):
                right[0, db] = shift_fast(mine_second, db)
            for da in range(slow):
                for db in range(fast):
                    if db:
                        left[da, db] = shift_fast(left[da, 0], db)
                    if da:
                        right[da, db] = shift_slow(right[0, db], da)
            order = [(da, db) for da in range(slow) for db in range(fast)]
            size = edges[i + 1] - edges[i]
            flat = jnp.concatenate([
                jnp.concatenate([left[at].reshape(share * size, half) for at in order], 0),
                jnp.concatenate([right[at].reshape(share * size, units - half) for at in order], 0),
            ], 1)
            cuts = LAST_CUTS if i == n - 1 else 1
            for j in range(cuts):
                lo, hi = width * j // cuts, width * (j + 1) // cuts
                sums = jnp.dot(flat, down_weight[:, lo:hi], preferred_element_type=jnp.float32).astype(jnp.bfloat16)
                sums = sums.reshape(n_col, share, size, hi - lo)
                total = lax.dynamic_index_in_dim(sums, part, 1, keepdims=False).astype(jnp.float32)
                for dk in range(1, share):
                    other = lax.dynamic_index_in_dim(sums, (part + dk) % share, 1, keepdims=False)
                    other = shift_part(other, dk)
                    total = total + other.astype(jnp.float32)
                total = total.astype(jnp.bfloat16)
                mine = lax.dynamic_index_in_dim(total, place(group), 0, keepdims=False).astype(jnp.float32)
                for dz in range(1, n_col):
                    block = lax.dynamic_index_in_dim(total, place((group + dz) % n_col), 0, keepdims=False)
                    block = shift_group(block, dz)
                    mine = mine + block.astype(jnp.float32)
                outs[i, j] = mine.astype(jnp.bfloat16)
        last = jnp.concatenate([outs[n - 1, j] for j in range(LAST_CUTS)], 1)
        whole = jnp.concatenate([outs[i, 0] for i in range(n - 1)] + [last], 0)
        return whole.reshape(seqs, own, width)

    return jax.shard_map(
        layer,
        mesh=mesh,
        in_specs=(P(None, "col", "row"), P(None, "col", "row"), P("row", "col")),
        out_specs=P(None, "row", "col"),
        check_vma=False,
    )
```
